32 devices in a mesh: section: 2 (over core), dp: 8 (over z, y), mp: 2 (over x).
Axes of the slice: x: 2, y: 2, z: 4, core: 2. Of those that a mesh axis runs over, the one named last changes fastest.
Arguments:
- hidden_in: bfloat16 [32, 512, 768], P('dp'), may hold values from -6 to 6
- segment_ids: int32 [32, 512], P('dp'), may hold values from 0 to 3, never falling along the last dimension, each value on 1 to 256 neighbouring positions
- cotangent: float32 [32, 512, 768], P('dp'), may hold values from -6 to 6
- w_proj: bfloat16 [2, 5, 768, 384], P('section', None, None, 'mp'), may hold values from -0.21875 to 0.21875
- w_depth: bfloat16 [2, 9, 768], P('section'), may hold values from -2 to 2
- w_kernel: bfloat16 [2, 384, 54], P('section', 'mp'), may hold values from -0.3125 to 0.3125
- w_out: bfloat16 [2, 2, 384, 768], P('section', None, 'mp'), may hold values from -0.625 to 0.625
- w_expand: bfloat16 [2, 2, 384, 1536], P('section', 'mp'), may hold values from -0.3125 to 0.3125
- shrink_weight: bfloat16 [2, 2, 1536, 384], P('section', 'mp'), may hold values from -0.21875 to 0.21875
- ln_gain: bfloat16 [2, 2, 768], P('section'), may hold values from 0.25 to 1.75
- ln_bias: bfloat16 [2, 2, 768], P('section'), may hold values from -3 to 3
Outputs:
- layer_outputs: bfloat16 [2, 32, 512, 768], P('section', 'dp')
- input_grads: float32 [2, 32, 512, 768], P('section', 'dp')
- proj_grad: float32 [2, 5, 768, 384], P('section', None, None, 'mp')
- depth_grad: float32 [2, 9, 768], P('section')
- kernel_grad: float32 [2, 384, 54], P('section', 'mp')
- out_grad: float32 [2, 2, 384, 768], P('section', None, 'mp')
- expand_grad: float32 [2, 2, 384, 1536], P('section', 'mp')
- shrink_grad: float32 [2, 2, 1536, 384], P('section', 'mp')
- gain_grad: float32 [2, 2, 768], P('section')
- bias_grad: float32 [2, 2, 768], P('section')
The draws below stay inside these ranges and needn't reach their ends.
Inputs may be any that keep to these rules, and one draw needn't show every extreme that they name: `segment_ids`: along each row the ids never fall; each row holds 4 documents of 1 to 256 consecutive tokens, and some row has a document of exactly 256 tokens.
All inputs are finite; a program needn't handle non-finite values.
Results may differ from the reference program's by a relative error of at most 0.025.
Values may be sent and summed in bfloat16 or wider, within the bound.
A program may use at most 320 MiB of HBM per device.

```python
import math
import jax
import jax.numpy as jnp
import numpy as np
from jax import lax

D = 768
ATT_HEADS = 6
HEAD = 64
KSIZE = 9
FF = 3072
GROUPS = 2
LEN = 512
DOCS = 4
ATT = 384
ROWS = 32
LAYERS = 2


def block_levels(rng, shape, cuts, least, top_value):
    gain = 1.0
    for dim, shards_of in cuts:
        steps = jax.random.uniform(jax.random.fold_in(jax.random.fold_in(rng, 6), dim), (shards_of,), jnp.float32, least / len(cuts), top_value / len(cuts))
        gain = gain * jnp.repeat(jnp.exp(steps), shape[dim] // shards_of).reshape((-1,) + (1,) * (len(shape) - 1 - dim))
    return gain


def split_up(amount, total, most, lean):
    weights = [(1 << 20) // math.isqrt(grade ** lean) + 1 for grade in range(2, amount + 1)]
    rest, given = total - most - (amount - 1), [1] * (amount - 1)
    while rest > 0:
        free = [i for i in range(amount - 1) if given[i] < most]
        whole, left = sum([weights[i] for i in free]), rest
        for i in free:
            extra = min(most - given[i], max(1, left * weights[i] // whole), rest)
            given[i] = given[i] + extra
            rest = rest - extra
    return np.array([most] + given)


def uneven(stream_key, amount, total, reach, slope):
    if amount == 2:
        one = jax.random.randint(stream_key, (), max(1, total - reach), min(reach, total - 1) + 1)
        return jnp.stack([one, total - one])
    sizes = jnp.asarray(split_up(amount, total, reach, slope), jnp.int32)
    couples = (amount - 1) // 2
    donor, sink = sizes[1:1 + 2 * couples:2], sizes[2:2 + 2 * couples:2]
    room = jnp.minimum(donor - 1, reach - sink)
    moved = jax.random.randint(jax.random.fold_in(stream_key, 1), (couples,), 0, 1 << 20) % (room + 1)
    sizes = sizes.at[1:1 + 2 * couples:2].set(donor - moved).at[2:2 + 2 * couples:2].set(sink + moved)
    return sizes[jax.random.permutation(jax.random.fold_in(stream_key, 2), amount)]


def centred(rng, extent, deviation, limit, cuts=(), held_as=jnp.bfloat16):
    loudness = block_levels(rng, extent, cuts, -0.22, 0.18) if cuts else 1.0
    array = jax.random.normal(rng, extent, jnp.float32) * deviation * loudness
    return jnp.minimum(jnp.maximum(array, -limit), limit).astype(held_as)


def setup_inputs(seed: int = 0) -> dict:
    keys = jax.random.split(jax.random.key(seed), 12)
    hidden_in = centred(keys[0], (ROWS, LEN, D), 1.0, 6.0, ((0, 8),))
    segment_ids = jax.vmap(lambda own: jnp.searchsorted(jnp.cumsum(uneven(own, DOCS, LEN, LEN // 2, 1)), jnp.arange(LEN), side="right"))(jax.random.split(keys[1], ROWS)).reshape((ROWS, LEN)).astype(jnp.int32)
    cotangent = centred(keys[2], (ROWS, LEN, D), 1.0, 6.0, ((0, 8),), jnp.float32)
    w_proj = centred(keys[3], (LAYERS, 5, D, ATT), D ** -0.5, 0.21875, ((0, 2), (3, 2)))
    w_depth = centred(keys[4], (LAYERS, KSIZE, D), KSIZE ** -0.5, 2.0, ((0, 2),))
    w_kernel = centred(keys[5], (LAYERS, ATT, ATT_HEADS * KSIZE), ATT ** -0.5, 0.3125, ((0, 2), (1, 2)))
    w_out = centred(keys[6], (LAYERS, 2, ATT, D), (ATT // 4) ** -0.5, 0.625, ((0, 2), (2, 2)))
    w_expand = centred(keys[7], (LAYERS, GROUPS, D // GROUPS, FF // GROUPS), (D // GROUPS) ** -0.5, 0.3125, ((0, 2), (1, 2)))
    shrink_weight = centred(keys[8], (LAYERS, GROUPS, FF // GROUPS, D // GROUPS), (FF // GROUPS // 2) ** -0.5, 0.21875, ((0, 2), (1, 2)))
    ln_gain = jnp.clip(1.0 + 0.15 * jax.random.normal(keys[9], (LAYERS, 2, D), jnp.float32), 0.25, 1.75).astype(jnp.bfloat16)
    ln_bias = centred(keys[10], (LAYERS, 2, D), 0.5, 3.0, ((0, 2),))
    return {"hidden_in": hidden_in, "segment_ids": segment_ids, "cotangent": cotangent, "w_proj": w_proj, "w_depth": w_depth, "w_kernel": w_kernel, "w_out": w_out, "w_expand": w_expand, "shrink_weight": shrink_weight, "ln_gain": ln_gain, "ln_bias": ln_bias}


EPS = 1e-05
FLOOR = -1000000000.0
HIGHEST_PRECISE = lax.Precision.HIGHEST

@jax.custom_vjp
def low(v):
    return lax.optimization_barrier(v.astype(jnp.bfloat16)).astype(jnp.float32)

@jax.custom_vjp
def lower_backward(v):
    return v

def low_keep(v):
    return (low(v), None)

def low_pass(kept, grad):
    return (grad,)

def back_keep(v):
    return (v, None)

def back_low(kept, grad):
    return (low(grad),)
low.defvjp(low_keep, low_pass)
lower_backward.defvjp(back_keep, back_low)

def shifted_masks(segment, tap_count):
    half_width = tap_count // 2
    padded = jnp.pad(segment, ((0, 0), (half_width, half_width)), constant_values=-1)
    sequence_length = segment.shape[1]
    return [lax.slice_in_dim(padded, offset, offset + sequence_length, axis=1) == segment for offset in range(tap_count)]

def expand_mask(tap_mask, target_rank):
    return tap_mask.reshape(tap_mask.shape + (1,) * (target_rank - 2))

def padded_rows(values, tap_count):
    half_width = tap_count // 2
    pad_spec = [(0, 0)] * values.ndim
    pad_spec[1] = (half_width, half_width)
    return jnp.pad(values, pad_spec)

def tap_take(values, tap_mask, offset, tap_count):
    window = lax.slice_in_dim(padded_rows(values, tap_count), offset, offset + values.shape[1], axis=1)
    return jnp.where(expand_mask(tap_mask, values.ndim), window, 0.0)

def norm_apply(summed, gain_row, bias_row):
    centered = summed - lax.optimization_barrier(jnp.mean(summed, axis=-1, keepdims=True))
    normed = centered * lax.rsqrt(lax.optimization_barrier(jnp.mean(centered * centered, axis=-1, keepdims=True)) + EPS)
    return normed * gain_row + bias_row

def layer_apply(inputs, segment, w_proj, w_depth, w_kernel, w_out, w_expand, shrink_weight, norm_gains, norm_biases):
    batch_row_count, sequence_length, hidden_width = inputs.shape
    tap_masks = shifted_masks(segment, KSIZE)
    inputs_low = low(inputs)
    projected = [lower_backward(jnp.einsum('bld,da->bla', inputs_low, w_proj[proj_index], precision=HIGHEST_PRECISE)) for proj_index in range(4)]
    depth_conv = jnp.zeros(inputs.shape, jnp.float32)
    for tap_index in range(KSIZE):
        depth_conv = depth_conv + tap_take(inputs, tap_masks[tap_index], tap_index, KSIZE) * w_depth[tap_index]
    key_conv = lower_backward(jnp.einsum('bld,da->bla', low(depth_conv), w_proj[4], precision=HIGHEST_PRECISE))
    product = key_conv * projected[0]
    logits = lower_backward(jnp.einsum('bla,ak->blk', low(product), w_kernel, precision=HIGHEST_PRECISE))
    kernel = jax.nn.softmax(logits.reshape(batch_row_count, sequence_length, ATT_HEADS, KSIZE), axis=-1)
    conv_value = projected[3].reshape(batch_row_count, sequence_length, ATT_HEADS, HEAD)
    conv_mixed = jnp.zeros(conv_value.shape, jnp.float32)
    for tap_index in range(KSIZE):
        conv_mixed = conv_mixed + kernel[..., tap_index, None] * tap_take(conv_value, tap_masks[tap_index], tap_index, KSIZE)
    queries_low = low(projected[0]).reshape(batch_row_count, sequence_length, ATT_HEADS, HEAD)
    keys_low = low(projected[1]).reshape(batch_row_count, sequence_length, ATT_HEADS, HEAD)
    values_low = low(projected[2]).reshape(batch_row_count, sequence_length, ATT_HEADS, HEAD)
    scores = lower_backward(HEAD ** (-0.5) * jnp.einsum('bqhd,bkhd->bhqk', queries_low, keys_low, precision=HIGHEST_PRECISE))
    same_doc = (segment[:, :, None] == segment[:, None, :])[:, None]
    attn_probs = jax.nn.softmax(jnp.where(same_doc, scores, FLOOR), axis=-1)
    context = jnp.einsum('bhqk,bkhd->bqhd', low(attn_probs), values_low, precision=HIGHEST_PRECISE)
    stacked = low(lower_backward(jnp.stack([context.reshape(batch_row_count, sequence_length, ATT), conv_mixed.reshape(batch_row_count, sequence_length, ATT)])))
    mixer_out = lower_backward(jnp.einsum('pbla,pad->bld', stacked, w_out, precision=HIGHEST_PRECISE))
    first_out = norm_apply(mixer_out + inputs, norm_gains[0], norm_biases[0])
    grouped = low(first_out.reshape(batch_row_count, sequence_length, GROUPS, hidden_width // GROUPS))
    hidden_pre = lower_backward(jnp.einsum('blgc,gcf->blgf', grouped, w_expand, precision=HIGHEST_PRECISE))
    active_lower_half = low(jax.nn.gelu(hidden_pre, approximate=False))
    feedforward_output = lower_backward(jnp.einsum('pjsa,sax->pjsx', active_lower_half, shrink_weight, precision=HIGHEST_PRECISE)).reshape(batch_row_count, sequence_length, hidden_width)
    return norm_apply(feedforward_output + first_out, norm_gains[1], norm_biases[1])

def reference(hidden_in, segment_ids, cotangent, w_proj, w_depth, w_kernel, w_out, w_expand, shrink_weight, ln_gain, ln_bias):
    params = tuple((tensor.astype(jnp.float32) for tensor in (w_proj, w_depth, w_kernel, w_out, w_expand, shrink_weight, ln_gain, ln_bias)))
    group_rows = math.gcd(ROWS, 8)
    group_count = ROWS // group_rows

    def grouped_view(tensor):
        return tensor.reshape((group_count, group_rows) + tensor.shape[1:])

    def forward(hidden, probe_zero, *weights):

        def one_group(pieces):
            rows_in, probe_in, segment = pieces
            first_layer = layer_apply(rows_in, segment, *[tensor[0] for tensor in weights])
            second_in = low(lower_backward(first_layer)) + probe_in
            second_layer = layer_apply(second_in, segment, *[tensor[1] for tensor in weights])
            return (second_layer, first_layer)
        second_all, first_all = lax.map(jax.checkpoint(one_group), (grouped_view(hidden), grouped_view(probe_zero), grouped_view(segment_ids)))
        return (second_all.reshape(ROWS, LEN, D), first_all.reshape(ROWS, LEN, D))
    hidden = hidden_in.astype(jnp.float32)
    probe_zero = jnp.zeros(hidden.shape, jnp.float32)
    second_out, pullback, first_out = jax.vjp(forward, hidden, probe_zero, *params, has_aux=True)
    grads_all = pullback(cotangent.astype(jnp.float32))
    layer_outputs = jnp.stack([first_out, second_out]).astype(jnp.bfloat16)
    input_grads = jnp.stack([grads_all[0], grads_all[1]])
    return (layer_outputs, input_grads, grads_all[2], grads_all[3], grads_all[4], grads_all[5], grads_all[6], grads_all[7], grads_all[8], grads_all[9])
```

```python
from functools import partial

import jax
import jax.numpy as jnp
from jax import lax
from jax.sharding import PartitionSpec as P

ATT_HEADS = 6
HEAD = 64
KSIZE = 9
EPS = 1e-05
FLOOR = -1000000000.0
BF = jnp.bfloat16
F32 = jnp.float32


def mm(a, b, dims):
    return lax.dot_general(a, b, (dims, ((), ())), preferred_element_type=F32)


def shift(values, by):
    length = values.shape[0]
    if by == 0:
        return values
    pad = ((max(-by, 0), max(by, 0)),) + ((0, 0),) * (values.ndim - 1)
    start = max(by, 0)
    return lax.slice_in_dim(jnp.pad(values, pad), start, start + length, axis=0)


def tap_masks(segment):
    half = KSIZE // 2
    padded = jnp.pad(segment, (half, half), constant_values=-1)
    length = segment.shape[0]
    return [
        (lax.slice_in_dim(padded, t, t + length) == segment)[:, None] for t in range(KSIZE)
    ]


def take(values, mask, t):
    return jnp.where(mask, shift(values, t - KSIZE // 2), 0.0)


def give(values, mask, t):
    return shift(jnp.where(mask, values, 0.0), KSIZE // 2 - t)


def norm_forward(summed, gain, bias):
    centered = summed - jnp.mean(summed, axis=-1, keepdims=True)
    inverse = lax.rsqrt(jnp.mean(centered * centered, axis=-1, keepdims=True) + EPS)
    normed = centered * inverse
    return normed * gain + bias, normed, inverse


def norm_backward(grad, normed, inverse, gain):
    u = grad * gain
    dz = inverse * (
        u
        - jnp.mean(u, axis=-1, keepdims=True)
        - normed * jnp.mean(u * normed, axis=-1, keepdims=True)
    )
    return dz, jnp.sum(grad * normed, axis=0), jnp.sum(grad, axis=0)


def heads_of(flat):
    return flat.reshape(flat.shape[0], ATT_HEADS, -1)


def layer_forward(x, segment, w):
    masks = tap_masks(segment)
    xb = x.astype(BF)
    proj = [mm(xb, w["proj"][p], ((1,), (0,))) for p in range(4)]
    depth = sum(take(x, masks[t], t) * w["depth"][t] for t in range(KSIZE))
    depth_low = depth.astype(BF)
    kc = mm(depth_low, w["proj"][4], ((1,), (0,)))
    prod_low = (kc * proj[0]).astype(BF)
    logits = mm(prod_low, w["kernel"], ((1,), (0,)))
    kern = jax.nn.softmax(heads_of(logits), axis=-1)
    cf = heads_of(proj[3])
    conv = sum(
        kern[..., t, None] * take(cf, masks[t][..., None], t) for t in range(KSIZE)
    )
    q, k, v = (heads_of(proj[p].astype(BF)) for p in range(3))
    scores = jnp.einsum("qhd,khd->hqk", q, k, preferred_element_type=F32) * HEAD**-0.5
    same = segment[:, None] == segment[None, :]
    probs = jax.nn.softmax(jnp.where(same, scores, FLOOR), axis=-1)
    ctx = jnp.einsum("hqk,khd->qhd", probs.astype(BF), v, preferred_element_type=F32)
    length = x.shape[0]
    cat = jnp.concatenate([ctx.reshape(length, -1), conv.reshape(length, -1)], axis=1).astype(BF)
    mixed = mm(cat, w["out"], ((1,), (0,)))
    y1, n0, s0 = norm_forward(mixed + x, w["gain"][0], w["bias"][0])
    groups, group_width, _ = w["expand"].shape
    grp = y1.astype(BF).reshape(length, groups, group_width)
    pre = jnp.einsum("lgc,gcf->glf", grp, w["expand"], preferred_element_type=F32)
    act = jax.nn.gelu(pre, approximate=False).astype(BF)
    ffn = jnp.einsum("glf,gfc->lgc", act, w["shrink"], preferred_element_type=F32)
    y2, n1, s1 = norm_forward(ffn.reshape(length, -1) + y1, w["gain"][1], w["bias"][1])
    kept = (x, proj, depth_low, kc, prod_low, kern, probs, cat, n0, s0, grp, pre, act, n1, s1)
    return y2.astype(BF), kept


def layer_backward(grad, segment, w, kept):
    x, proj, depth_low, kc, prod_low, kern, probs, cat, n0, s0, grp, pre, act, n1, s1 = kept
    length = x.shape[0]
    masks = tap_masks(segment)
    dz2, gain1, bias1 = norm_backward(grad, n1, s1, w["gain"][1])
    dffn = dz2.astype(BF).reshape(grp.shape)
    shrink_grad = jnp.einsum("glf,lgc->gfc", act, dffn, preferred_element_type=F32)
    dact = jnp.einsum("lgc,gfc->glf", dffn, w["shrink"], preferred_element_type=F32)
    dpre = jax.vjp(partial(jax.nn.gelu, approximate=False), pre)[1](dact)[0].astype(BF)
    expand_grad = jnp.einsum("lgc,glf->gcf", grp, dpre, preferred_element_type=F32)
    dgrp = jnp.einsum("glf,gcf->lgc", dpre, w["expand"], preferred_element_type=F32)
    dy1 = dz2 + dgrp.reshape(length, -1)
    dz1, gain0, bias0 = norm_backward(dy1, n0, s0, w["gain"][0])
    dmix = dz1.astype(BF)
    out_grad = mm(cat, dmix, ((0,), (0,)))
    dcat = mm(dmix, w["out"], ((1,), (1,))).astype(BF)
    half = dcat.shape[1] // 2
    dctx, dconv = heads_of(dcat[:, :half]), heads_of(dcat[:, half:]).astype(F32)
    q, k, v = (heads_of(proj[p].astype(BF)) for p in range(3))
    dprobs = jnp.einsum("qhd,khd->hqk", dctx, v, preferred_element_type=F32)
    row_dot = jnp.sum(probs * dprobs, axis=-1, keepdims=True)
    dscores = (probs * (dprobs - row_dot)).astype(BF)
    dq_att = jnp.einsum("hqk,khd->qhd", dscores, k, preferred_element_type=F32) * HEAD**-0.5
    dk = jnp.einsum("hqk,qhd->khd", dscores, q, preferred_element_type=F32) * HEAD**-0.5
    dv = jnp.einsum("hqk,qhd->khd", probs.astype(BF), dctx, preferred_element_type=F32)
    cf = heads_of(proj[3])
    dkern, dc = [], 0.0
    for t in range(KSIZE):
        mask = masks[t][..., None]
        dkern.append(jnp.sum(dconv * take(cf, mask, t), axis=-1))
        dc = dc + give(kern[..., t, None] * dconv, mask, t)
    dkern = jnp.stack(dkern, axis=-1)
    dlogits = kern * (dkern - jnp.sum(kern * dkern, axis=-1, keepdims=True))
    dlogits = dlogits.reshape(length, -1).astype(BF)
    kernel_grad = mm(prod_low, dlogits, ((0,), (0,)))
    dprod = mm(dlogits, w["kernel"], ((1,), (1,)))
    dkc = (dprod * proj[0]).astype(BF)
    dq = (dq_att.reshape(length, -1) + dprod * kc).astype(BF)
    ddepth = mm(dkc, w["proj"][4], ((1,), (1,)))
    depth_grad, dxd = [], 0.0
    for t in range(KSIZE):
        depth_grad.append(jnp.sum(ddepth * take(x, masks[t], t), axis=0))
        dxd = dxd + give(ddepth * w["depth"][t], masks[t], t)
    flat = lambda value: value.reshape(length, -1).astype(BF)
    dproj = [dq, flat(dk), flat(dv), flat(dc)]
    xb = x.astype(BF)
    proj_grad = jnp.stack(
        [mm(xb, one, ((0,), (0,))) for one in dproj] + [mm(depth_low, dkc, ((0,), (0,)))]
    )
    dx = dz1 + dxd + sum(mm(one, w["proj"][p], ((1,), (1,))) for p, one in enumerate(dproj))
    small = (
        jnp.stack(depth_grad),
        kernel_grad,
        jnp.stack([gain0, gain1]),
        jnp.stack([bias0, bias1]),
    )
    return dx, (proj_grad, out_grad, expand_grad, shrink_grad), small


def swap(value, axis):
    return lax.ppermute(value, axis, [(0, 1), (1, 0)])


def by_section(first, second):
    section = lax.axis_index("section")
    own = jnp.where(section == 0, first, second)
    other = swap(jnp.where(section == 0, second, first), "section")
    return jnp.where(section == 0, own, other), jnp.where(section == 0, other, own)


def on_device(
    hidden_in, segment_ids, cotangent, w_proj, w_depth, w_kernel, w_out, w_expand, shrink_weight,
    ln_gain, ln_bias,
):
    section, half = lax.axis_index("section"), lax.axis_index("mp")
    row = half * 2 + section

    def own_row(value):
        return lax.dynamic_index_in_dim(value, row, 0, keepdims=False)

    def whole(value, axis):
        if axis is not None:
            value = lax.all_gather(value, "mp", axis=axis, tiled=True)
        return lax.all_gather(value, "section", axis=0, tiled=True)

    proj = whole(w_proj, 3)
    out = whole(w_out, 2)
    expand = whole(w_expand, 1)
    shrink = whole(shrink_weight, 1)
    kernel = whole(w_kernel, 1)
    depth = whole(w_depth, None)
    gain = whole(ln_gain, None)
    bias = whole(ln_bias, None)
    weights = [
        dict(
            proj=proj[layer],
            out=out[layer].reshape(-1, out.shape[-1]),
            expand=expand[layer],
            shrink=shrink[layer],
            kernel=kernel[layer],
            depth=depth[layer].astype(F32),
            gain=gain[layer].astype(F32),
            bias=bias[layer].astype(F32),
        )
        for layer in range(2)
    ]
    segment = own_row(segment_ids)
    x0 = own_row(hidden_in).astype(F32)
    out0, kept0 = layer_forward(x0, segment, weights[0])
    out1, kept1 = layer_forward(out0.astype(F32), segment, weights[1])
    outputs = jnp.stack(by_section(out0, out1))
    outputs = lax.all_gather(outputs, "mp", axis=0, tiled=True)

    def reduced(grads):
        proj_grad, out_grad, expand_grad, shrink_grad = (g.astype(BF) for g in grads)
        width = proj_grad.shape[2] // 2
        parts = (
            (proj_grad, 1, 2),
            (out_grad.reshape(2, -1, out_grad.shape[-1]), 2, 1),
            (expand_grad, 2, 0),
            (shrink_grad, 2, 0),
        )
        done = []
        for value, piece_axis, half_axis in parts:
            value = lax.psum_scatter(
                value, "section", scatter_dimension=piece_axis, tiled=True
            )
            value = lax.psum_scatter(value, "mp", scatter_dimension=half_axis, tiled=True)
            done.append(lax.psum(value, "dp"))
        return done

    dx1, grads1, small1 = layer_backward(own_row(cotangent), segment, weights[1], kept1)
    big1 = reduced(grads1)
    g0 = dx1.astype(BF)
    dx0, grads0, small0 = layer_backward(g0.astype(F32), segment, weights[0], kept0)
    big0 = reduced(grads0)
    input_grads = jnp.stack(by_section(dx0.astype(BF), g0))
    input_grads = lax.all_gather(input_grads, "mp", axis=0, tiled=True).astype(F32)
    big = []
    for first, second, axis in zip(big0, big1, (1, 2, 2, 2)):
        big.append(jnp.concatenate(by_section(first, second), axis=axis)[None].astype(F32))
    small = lax.psum((small0, small1), ("section", "mp", "dp"))
    depth_grad, kernel_grad, gain_grad, bias_grad = (
        jnp.where(section == 0, a, b) for a, b in zip(*small)
    )
    kernel_half = kernel_grad.shape[0] // 2
    kernel_grad = lax.dynamic_slice_in_dim(kernel_grad, half * kernel_half, kernel_half, 0)
    return (
        outputs[None],
        input_grads[None],
        big[0],
        depth_grad[None],
        kernel_grad[None],
        big[1],
        big[2],
        big[3],
        gain_grad[None],
        bias_grad[None],
    )


def solution(mesh):
    in_specs = (
        P("dp", None, None),
        P("dp", None),
        P("dp", None, None),
        P("section", None, None, "mp"),
        P("section", None, None),
        P("section", "mp", None),
        P("section", None, "mp", None),
        P("section", "mp", None, None),
        P("section", "mp", None, None),
        P("section", None, None),
        P("section", None, None),
    )
    out_specs = (
        P("section", "dp", None, None),
        P("section", "dp", None, None),
        P("section", None, None, "mp"),
        P("section", None, None),
        P("section", "mp", None),
        P("section", None, "mp", None),
        P("section", "mp", None, None),
        P("section", "mp", None, None),
        P("section", None, None),
        P("section", None, None),
    )
    return jax.shard_map(
        on_device, mesh=mesh, in_specs=in_specs, out_specs=out_specs, check_vma=False
    )
```

```python
from functools import partial

import jax
import jax.numpy as jnp
from jax import lax
from jax.sharding import PartitionSpec as P

ATT_HEADS = 6
HEAD = 64
KSIZE = 9
EPS = 1e-05
FLOOR = -1000000000.0
BF = jnp.bfloat16
F32 = jnp.float32


def mm(a, b, dims):
    return lax.dot_general(a, b, (dims, ((), ())), preferred_element_type=F32)


def shift(values, by):
    length = values.shape[0]
    if by == 0:
        return values
    pad = ((max(-by, 0), max(by, 0)),) + ((0, 0),) * (values.ndim - 1)
    start = max(by, 0)
    return lax.slice_in_dim(jnp.pad(values, pad), start, start + length, axis=0)


def tap_masks(segment):
    half = KSIZE // 2
    padded = jnp.pad(segment, (half, half), constant_values=-1)
    length = segment.shape[0]
    return [
        (lax.slice_in_dim(padded, t, t + length) == segment)[:, None] for t in range(KSIZE)
    ]


def take(values, mask, t):
    return jnp.where(mask, shift(values, t - KSIZE // 2), 0.0)


def give(values, mask, t):
    return shift(jnp.where(mask, values, 0.0), KSIZE // 2 - t)


def norm_forward(summed, gain, bias):
    centered = summed - jnp.mean(summed, axis=-1, keepdims=True)
    inverse = lax.rsqrt(jnp.mean(centered * centered, axis=-1, keepdims=True) + EPS)
    normed = centered * inverse
    return normed * gain + bias, normed, inverse


def norm_backward(grad, normed, inverse, gain):
    u = grad * gain
    dz = inverse * (
        u
        - jnp.mean(u, axis=-1, keepdims=True)
        - normed * jnp.mean(u * normed, axis=-1, keepdims=True)
    )
    return dz, jnp.sum(grad * normed, axis=0), jnp.sum(grad, axis=0)


def heads_of(flat):
    return flat.reshape(flat.shape[0], ATT_HEADS, -1)


def layer_forward(x, segment, w):
    masks = tap_masks(segment)
    xb = x.astype(BF)
    proj = [mm(xb, w["proj"][p], ((1,), (0,))) for p in range(4)]
    depth = sum(take(x, masks[t], t) * w["depth"][t] for t in range(KSIZE))
    depth_low = depth.astype(BF)
    kc = mm(depth_low, w["proj"][4], ((1,), (0,)))
    prod_low = (kc * proj[0]).astype(BF)
    logits = mm(prod_low, w["kernel"], ((1,), (0,)))
    kern = jax.nn.softmax(heads_of(logits), axis=-1)
    cf = heads_of(proj[3])
    conv = sum(
        kern[..., t, None] * take(cf, masks[t][..., None], t) for t in range(KSIZE)
    )
    q, k, v = (heads_of(proj[p].astype(BF)) for p in range(3))
    scores = jnp.einsum("qhd,khd->hqk", q, k, preferred_element_type=F32) * HEAD**-0.5
    same = segment[:, None] == segment[None, :]
    probs = jax.nn.softmax(jnp.where(same, scores, FLOOR), axis=-1)
    ctx = jnp.einsum("hqk,khd->qhd", probs.astype(BF), v, preferred_element_type=F32)
    length = x.shape[0]
    cat = jnp.concatenate([ctx.reshape(length, -1), conv.reshape(length, -1)], axis=1).astype(BF)
    mixed = mm(cat, w["out"], ((1,), (0,)))
    y1, n0, s0 = norm_forward(mixed + x, w["gain"][0], w["bias"][0])
    groups, group_width, _ = w["expand"].shape
    grp = y1.astype(BF).reshape(length, groups, group_width)
    pre = jnp.einsum("lgc,gcf->glf", grp, w["expand"], preferred_element_type=F32)
    act = jax.nn.gelu(pre, approximate=False).astype(BF)
    ffn = jnp.einsum("glf,gfc->lgc", act, w["shrink"], preferred_element_type=F32)
    y2, n1, s1 = norm_forward(ffn.reshape(length, -1) + y1, w["gain"][1], w["bias"][1])
    kept = (x, proj, depth_low, kc, prod_low, kern, probs, cat, n0, s0, grp, pre, act, n1, s1)
    return y2.astype(BF), kept


def layer_backward(grad, segment, w, kept):
    x, proj, depth_low, kc, prod_low, kern, probs, cat, n0, s0, grp, pre, act, n1, s1 = kept
    length = x.shape[0]
    masks = tap_masks(segment)
    dz2, gain1, bias1 = norm_backward(grad, n1, s1, w["gain"][1])
    dffn = dz2.astype(BF).reshape(grp.shape)
    shrink_grad = jnp.einsum("lgc,glf->gcf", dffn, act, preferred_element_type=F32)
    dact = jnp.einsum("lgc,gfc->glf", dffn, w["shrink"], preferred_element_type=F32)
    dpre = jax.vjp(partial(jax.nn.gelu, approximate=False), pre)[1](dact)[0].astype(BF)
    expand_grad = jnp.einsum("lgc,glf->gcf", grp, dpre, preferred_element_type=F32)
    dgrp = jnp.einsum("glf,gcf->lgc", dpre, w["expand"], preferred_element_type=F32)
    dy1 = dz2 + dgrp.reshape(length, -1)
    dz1, gain0, bias0 = norm_backward(dy1, n0, s0, w["gain"][0])
    dmix = dz1.astype(BF)
    out_grad = mm(cat, dmix, ((0,), (0,)))
    dcat = mm(dmix, w["out"], ((1,), (1,))).astype(BF)
    half = dcat.shape[1] // 2
    dctx, dconv = heads_of(dcat[:, :half]), heads_of(dcat[:, half:]).astype(F32)
    q, k, v = (heads_of(proj[p].astype(BF)) for p in range(3))
    dprobs = jnp.einsum("qhd,khd->hqk", dctx, v, preferred_element_type=F32)
    row_dot = jnp.sum(probs * dprobs, axis=-1, keepdims=True)
    dscores = (probs * (dprobs - row_dot)).astype(BF)
    dq_att = jnp.einsum("hqk,khd->qhd", dscores, k, preferred_element_type=F32) * HEAD**-0.5
    dk = jnp.einsum("hqk,qhd->khd", dscores, q, preferred_element_type=F32) * HEAD**-0.5
    dv = jnp.einsum("hqk,qhd->khd", probs.astype(BF), dctx, preferred_element_type=F32)
    cf = heads_of(proj[3])
    dkern, dc = [], 0.0
    for t in range(KSIZE):
        mask = masks[t][..., None]
        dkern.append(jnp.sum(dconv * take(cf, mask, t), axis=-1))
        dc = dc + give(kern[..., t, None] * dconv, mask, t)
    dkern = jnp.stack(dkern, axis=-1)
    dlogits = kern * (dkern - jnp.sum(kern * dkern, axis=-1, keepdims=True))
    dlogits = dlogits.reshape(length, -1).astype(BF)
    kernel_grad = mm(prod_low, dlogits, ((0,), (0,)))
    dprod = mm(dlogits, w["kernel"], ((1,), (1,)))
    dkc = (dprod * proj[0]).astype(BF)
    dq = (dq_att.reshape(length, -1) + dprod * kc).astype(BF)
    ddepth = mm(dkc, w["proj"][4], ((1,), (1,)))
    depth_grad, dxd = [], 0.0
    for t in range(KSIZE):
        depth_grad.append(jnp.sum(ddepth * take(x, masks[t], t), axis=0))
        dxd = dxd + give(ddepth * w["depth"][t], masks[t], t)
    flat = lambda value: value.reshape(length, -1).astype(BF)
    dproj = [dq, flat(dk), flat(dv), flat(dc)]
    xb = x.astype(BF)
    attention_grad = [mm(one, xb, ((0,), (0,))) for one in dproj]
    attention_grad += [mm(dkc, depth_low, ((0,), (0,))), out_grad[:half], out_grad[half:]]
    dx = dz1 + dxd + sum(mm(one, w["proj"][p], ((1,), (1,))) for p, one in enumerate(dproj))
    small = (
        jnp.stack(depth_grad),
        kernel_grad,
        jnp.stack([gain0, gain1]),
        jnp.stack([bias0, bias1]),
    )
    big = jnp.stack(attention_grad), jnp.concatenate([expand_grad[None], shrink_grad[None]])
    return dx, big, small


def swap(value, axis):
    return lax.ppermute(value, axis, [(0, 1), (1, 0)])


def by_section(first, second):
    section = lax.axis_index("section")
    own = jnp.where(section == 0, first, second)
    other = swap(jnp.where(section == 0, second, first), "section")
    return in_order(own, other, "section")


def in_order(own, other, axis):
    first = lax.axis_index(axis) == 0
    return jnp.where(first, own, other), jnp.where(first, other, own)


def pick(value, index, axis):
    return lax.dynamic_index_in_dim(value, index, axis, keepdims=False)


def both_halves(value, axis, cut):
    section = lax.axis_index("section")
    size = value.shape[cut] // 2
    piece = lax.dynamic_slice_in_dim(value, section * size, size, cut)
    came = swap(piece, "mp")
    other = jnp.concatenate(in_order(came, swap(came, "section"), "section"), axis=cut)
    return jnp.concatenate(in_order(value, other, "mp"), axis=axis)


def scattered(value):
    section, half = lax.axis_index("section"), lax.axis_index("mp")
    came = swap(pick(value, 1 - section, 2), "section")
    value = (pick(value, section, 2).astype(F32) + came.astype(F32)).astype(BF)
    came = swap(pick(value, 1 - half, 1), "mp")
    return pick(value, half, 1).astype(F32) + came.astype(F32)


def ring_sum(value):
    count = lax.axis_size("dp")
    order = [0, 2, 4, 6, 7, 5, 3, 1] if count == 8 else list(range(count))
    pairs = []
    for at in range(count):
        here, following = order[at], order[(at + 1) % count]
        pairs += [(here, following), (count + following, count + here)]
    place = jnp.asarray([order.index(at) for at in range(count)])[lax.axis_index("dp")]
    place = jnp.where(lax.axis_index("section") == 0, place, count - 1 - place)

    def send(block):
        return lax.ppermute(block, ("section", "dp"), pairs)

    blocks = value.reshape(count, -1, value.shape[-1])
    now = pick(blocks, place, 0)
    for step in range(1, count):
        term = pick(blocks, (place - step) % count, 0)
        now = (send(now).astype(F32) + term.astype(F32)).astype(BF)
    summed = lax.dynamic_update_index_in_dim(blocks, now, (place + 1) % count, 0)
    for step in range(count - 1):
        now = send(now)
        summed = lax.dynamic_update_index_in_dim(summed, now, (place - step) % count, 0)
    return summed.reshape(value.shape)


def to_owner(value, owner):
    pair = jnp.stack(in_order(value, swap(value, "section"), "section"))
    a, b = owner * 2, owner * 2 + 1
    other = lax.ppermute(pair, ("section", "mp"), [(a, b), (b, a)])
    return jnp.concatenate(in_order(pair, other, "mp"))


def on_device(
    hidden_in, segment_ids, cotangent, w_proj, w_depth, w_kernel, w_out, w_expand, shrink_weight,
    ln_gain, ln_bias,
):
    section, half = lax.axis_index("section"), lax.axis_index("mp")
    row = half * 2 + section

    def own_row(value):
        return lax.dynamic_index_in_dim(value, row, 0, keepdims=False)

    def layers(value):
        return in_order(value[0], swap(value[0], "section"), "section")

    fine = layers(jnp.concatenate([w_depth, ln_gain, ln_bias], axis=1))
    parts = [layers(value) for value in (w_proj, w_kernel, w_out, w_expand, shrink_weight)]
    weights = []
    for layer in range(2):
        proj, kernel, out, expand, shrink = (part[layer] for part in parts)
        vectors = fine[layer].astype(F32)
        out = both_halves(out, 1, 1)
        weights.append(
            dict(
                proj=both_halves(proj, 2, 1),
                out=out.reshape(-1, out.shape[-1]),
                expand=both_halves(expand, 0, 1),
                shrink=both_halves(shrink, 0, 1),
                kernel=both_halves(kernel, 0, 0),
                depth=vectors[:KSIZE],
                gain=vectors[KSIZE : KSIZE + 2],
                bias=vectors[KSIZE + 2 :],
            )
        )
    segment = own_row(segment_ids)
    x0 = own_row(hidden_in).astype(F32)
    out0, kept0 = layer_forward(x0, segment, weights[0])
    out1, kept1 = layer_forward(out0.astype(F32), segment, weights[1])
    pair = jnp.stack(by_section(out0, out1))
    outputs = jnp.concatenate(in_order(pair, swap(pair, "mp"), "mp"))

    def reduced(big, small, before):
        attention, feed = big
        wide = attention.shape[-1]
        attention = attention.astype(BF).reshape(attention.shape[0], 2, 2, -1, wide)
        feed = feed.astype(BF).reshape(feed.shape[0], 2, 2, -1, feed.shape[-1])
        feed = scattered(feed).astype(BF)
        if before is not None:
            feed, _ = lax.optimization_barrier((feed, before))
        feed = lax.psum(feed, "dp")
        depth_grad, kernel_grad, gain_grad, bias_grad = small
        packed = jnp.concatenate(
            [depth_grad, gain_grad, bias_grad, kernel_grad.reshape(-1, wide)]
        )
        packed = packed + swap(packed, "section")
        packed = packed + swap(packed, "mp")
        attention = scattered(attention)
        shape, count = attention.shape, attention.shape[0] * attention.shape[1]
        joined = jnp.concatenate([attention.reshape(count, wide), packed]).astype(BF)
        if before is None:
            joined, feed = lax.optimization_barrier((joined, feed))
            joined = lax.psum(joined, "dp")
        elif lax.axis_size("dp") == 8:
            joined = ring_sum(joined)
        else:
            joined, feed = lax.optimization_barrier((joined, feed))
            joined = lax.psum(joined, "dp")
        return joined[:count].reshape(shape), feed, joined[count:]

    dx1, big1, small1 = layer_backward(own_row(cotangent), segment, weights[1], kept1)
    done1 = reduced(big1, small1, None)
    g0 = dx1.astype(BF)
    grads_1 = to_owner(g0, 1)
    dx0, big0, small0 = layer_backward(g0.astype(F32), segment, weights[0], kept0)
    done0 = reduced(big0, small0, done1[0])
    grads_0 = to_owner(dx0.astype(BF), 0)
    input_grads = jnp.where(section == 0, grads_0, grads_1).astype(F32)
    attention = jnp.concatenate(by_section(done0[0], done1[0]), axis=1).astype(F32)
    feed = jnp.concatenate(by_section(done0[1], done1[1]), axis=1).astype(F32)
    packed = jnp.where(section == 0, done0[2], done1[2]).astype(F32)
    kernel_shape = weights[0]["kernel"].shape
    kernel_grad = packed[KSIZE + 4 :].reshape(kernel_shape)
    kernel_half = kernel_shape[0] // 2
    kernel_grad = lax.dynamic_slice_in_dim(kernel_grad, half * kernel_half, kernel_half, 0)
    return (
        outputs[None],
        input_grads[None],
        attention[:5].transpose(0, 2, 1)[None],
        packed[None, :KSIZE],
        kernel_grad[None],
        attention[5:][None],
        feed[0][None, None],
        feed[1].T[None, None],
        packed[None, KSIZE : KSIZE + 2],
        packed[None, KSIZE + 2 : KSIZE + 4],
    )


def solution(mesh):
    in_specs = (
        P("dp", None, None),
        P("dp", None),
        P("dp", None, None),
        P("section", None, None, "mp"),
        P("section", None, None),
        P("section", "mp", None),
        P("section", None, "mp", None),
        P("section", "mp", None, None),
        P("section", "mp", None, None),
        P("section", None, None),
        P("section", None, None),
    )
    out_specs = (
        P("section", "dp", None, None),
        P("section", "dp", None, None),
        P("section", None, None, "mp"),
        P("section", None, None),
        P("section", "mp", None),
        P("section", None, "mp", None),
        P("section", "mp", None, None),
        P("section", "mp", None, None),
        P("section", None, None),
        P("section", None, None),
    )
    return jax.shard_map(
        on_device, mesh=mesh, in_specs=in_specs, out_specs=out_specs, check_vma=False
    )
```
